32 devices in a mesh: grp: 2 (over y), row: 4 (over x, core), col: 4 (over z).
Axes of the slice: x: 2, y: 2, z: 4, core: 2. Of those that a mesh axis runs over, the one named last changes fastest.
Arguments:
- perturbation: bfloat16 [4, 12000, 12000], P('grp', 'row', 'col'), parts along dimension 0, may hold values from -96 to 96
- occ_coeffs: bfloat16 [12000, 2000], P('row', 'col'), may hold values from -0.0546875 to 0.0546875
- vir_coeffs: bfloat16 [12000, 512], P('col', 'row'), may hold values from -0.0546875 to 0.0546875
- occ_energies: float32 [2000], replicated, may hold values from -1 to -0.1
- vir_energies: float32 [512], replicated, may hold values from 0.1 to 1.5
Outputs:
- density_response: bfloat16 [4, 12000, 12000], P('grp', 'row', 'col'), parts along dimension 0
The draws below stay inside these ranges and needn't reach their ends.
There are 2 independent parts, one for each index of `grp`. The reference program is written for one: setup_inputs(seed, part) draws one part's arguments, and reference() takes and returns one part's arrays. A program takes and returns all parts, laid end to end along the dimension named above; an argument that names none is the same for every part. Nothing has to cross between parts.
All inputs are finite; a program needn't handle non-finite values.
Results may differ from the reference program's by a relative error of at most 0.0098.
Values may be sent and summed in bfloat16 or wider, within the bound.
A program may use at most 192 MiB of HBM per device.

```python
import jax
import jax.numpy as jnp
from jax import lax

NB = 12000
NOCC = 2000
NV = 512
PERT = 2


def block_levels(rng, shape, cuts, smallest, high):
    factor_of = 1.0
    for dim, shards_of in cuts:
        draws = jax.random.uniform(jax.random.fold_in(jax.random.fold_in(rng, 6), dim), (shards_of,), jnp.float32, smallest / len(cuts), high / len(cuts))
        factor_of = factor_of * jnp.repeat(jnp.exp(draws), shape[dim] // shards_of).reshape((-1,) + (1,) * (len(shape) - 1 - dim))
    return factor_of


def scatter_about(key, shape, spread, bound, cuts=(), held_as=jnp.bfloat16):
    array = spread * jax.random.normal(key, shape, jnp.float32)
    if cuts:
        array = array * block_levels(key, shape, cuts, -0.22, 0.18)
    return jnp.clip(array, -bound, bound).astype(held_as)


def setup_inputs(seed: int = 0, part: int = 0) -> dict:
    seeds = jax.random.split(jax.random.key(seed), 6)
    part_keys = jax.random.split(jax.random.fold_in(seeds[5], part), 6)
    return {
        "perturbation": scatter_about(part_keys[0], (PERT, NB, NB), 16.0, 96.0, ((1, 4), (2, 4))),
        "occ_coeffs": scatter_about(seeds[1], (NB, NOCC), NB ** -0.5, 0.0546875, ((0, 4), (1, 4))),
        "vir_coeffs": scatter_about(seeds[2], (NB, NV), NB ** -0.5, 0.0546875, ((0, 4), (1, 4))),
        "occ_energies": jnp.clip(jax.random.uniform(seeds[3], (NOCC,), jnp.float32, -1.0, -0.1), -1.0, -0.1),
        "vir_energies": jnp.clip(jax.random.uniform(seeds[4], (NV,), jnp.float32, 0.1, 1.5), 0.1, 1.5),
    }


def reference(perturbation, occ_coeffs, vir_coeffs, occ_energies, vir_energies):
    gaps = occ_energies[:, None] - vir_energies[None, :]
    occ_wide = occ_coeffs.astype(jnp.float32)
    results = []
    for index in range(PERT):
        image = jnp.dot(perturbation[index], vir_coeffs, preferred_element_type=jnp.float32)
        coupling = jnp.dot(occ_wide.T, image, precision=lax.Precision.HIGHEST)
        response = (coupling / gaps).astype(jnp.bfloat16)
        mixed = jnp.dot(occ_coeffs, response, preferred_element_type=jnp.float32).astype(jnp.bfloat16)
        results.append(jnp.dot(mixed, vir_coeffs.T, preferred_element_type=jnp.float32).astype(jnp.bfloat16))
    return jnp.stack(results)
```

```python
import jax
import jax.numpy as jnp
from jax import lax
from jax.sharding import PartitionSpec as P

BF16 = jnp.bfloat16
F32 = jnp.float32


def per_device(perturbation, occ_coeffs, vir_coeffs, occ_energies, vir_energies):
    vir_rows = lax.all_gather(vir_coeffs, "row", axis=1, tiled=True)
    occ_parts = lax.all_gather(occ_coeffs, "col")
    cols, _, width = occ_parts.shape
    image = jnp.einsum(
        "pij,jv->piv", perturbation, vir_rows, preferred_element_type=F32
    ).astype(BF16)
    part = jnp.einsum("cio,piv->pcov", occ_parts, image, preferred_element_type=F32).astype(BF16)
    coupling = lax.psum(part, ("row", "col"))
    gaps = occ_energies.reshape(cols, width)[:, :, None] - vir_energies[None, None, :]
    response = (coupling.astype(F32) / gaps[None]).astype(BF16)
    mixed = jnp.einsum("cio,pcov->piv", occ_parts, response, preferred_element_type=F32).astype(BF16)
    return jnp.einsum("piv,jv->pij", mixed, vir_rows, preferred_element_type=F32).astype(BF16)


def solution(mesh):
    placed = (P("grp", "row", "col"), P("row", "col"), P("col", "row"), P(), P())
    return jax.shard_map(
        per_device, mesh=mesh, in_specs=placed, out_specs=P("grp", "row", "col"), check_vma=False
    )
```
